32 devices in a mesh: dp: 16 (over z, x, core), stream: 2 (over y).
Axes of the slice: x: 2, y: 2, z: 4, core: 2. Of those that a mesh axis runs over, the one named last changes fastest.
Arguments:
- tokens: bfloat16 [80, 2, 200, 768], P('dp', 'stream'), may hold values from -6 to 6
- text_segment: int32 [80, 200], P('dp'), may hold values from 0 to 5, as said below
- ln1_gain: float32 [768], replicated, may hold values from 0.5 to 1.5
- ln1_bias: float32 [768], replicated, may hold values from -3 to 3
- qkv_weight: bfloat16 [768, 2304], replicated, may hold values from -0.3125 to 0.3125
- out_weight: bfloat16 [768, 768], replicated, may hold values from -0.625 to 0.625
- attn_scale: float32 [768], replicated, may hold values from 0.25 to 1.75
- ffn_scale: float32 [768], replicated, may hold values from 0.25 to 1.75
- ln2_gain: float32 [2, 768], P('stream'), may hold values from 0.5 to 1.5
- ln2_bias: float32 [2, 768], P('stream'), may hold values from -3 to 3
- expert_in: bfloat16 [2, 768, 3072], P('stream'), may hold values from -0.21875 to 0.21875
- expert_out: bfloat16 [2, 3072, 768], P('stream'), may hold values from -0.15625 to 0.15625
- out_cot: bfloat16 [80, 2, 200, 768], P('dp', 'stream'), may hold values from -6 to 6
Outputs:
- block_out: bfloat16 [80, 2, 200, 768], P('dp', 'stream')
- tokens_grad: bfloat16 [80, 2, 200, 768], P('dp', 'stream')
- ln1_gain_grad: float32 [768], replicated
- ln1_bias_grad: float32 [768], replicated
- qkv_weight_grad: float32 [768, 2304], replicated
- out_weight_grad: float32 [768, 768], replicated
- attn_scale_grad: float32 [768], replicated
- ffn_scale_grad: float32 [768], replicated
- ln2_gain_grad: float32 [2, 768], P('stream')
- ln2_bias_grad: float32 [2, 768], P('stream')
- expert_in_grad: float32 [2, 768, 3072], P('stream')
- expert_out_grad: float32 [2, 3072, 768], P('stream')
The draws below stay inside these ranges and needn't reach their ends.
Inputs may be any that keep to these rules, and one draw needn't show every extreme that they name: `text_segment`: in each group the text slots hold the captions numbered below 5 in order, each of 1 to 39 slots, followed by padding slots numbered 5.
All inputs are finite; a program needn't handle non-finite values.
Results may differ from the reference program's by a relative error of at most 0.015.
The reference program's roundings to bfloat16 on the way count: a program that leaves them out, or rounds other values in their place, can miss the bound.
Values may be sent and summed in bfloat16 or wider, within the bound.
A program may use at most 256 MiB of HBM per device.

```python
import jax
import jax.numpy as jnp
from jax import lax

D = 768
HEADS = 12
HDIM = 64
FF = 3072
SLOTS = 200
PATCHES = 197
CAPTIONS = 5
CAP_MAX = 39
G_DEV = 5
GROUPS = 80


def draw_text_segment(key, part):
    lengths = jax.random.randint(key, (GROUPS, CAPTIONS), 1, CAP_MAX + 1).astype(jnp.int32)
    caption_ends = jnp.cumsum(lengths, axis=1).astype(jnp.int32)
    slot_index = jnp.arange(SLOTS, dtype=jnp.int32)
    passed = (slot_index[None, :, None] >= caption_ends[:, None, :]).astype(jnp.int32)
    return jnp.sum(passed, axis=2).astype(jnp.int32)


def level_of(own_key, shape, shards, low, top_value):
    level, own = 1.0, jax.random.fold_in(own_key, 6)
    for position, blocks in shards:
        heights = jnp.exp(jax.random.uniform(jax.random.fold_in(own, position), (blocks,), jnp.float32, low / len(shards), top_value / len(shards)))
        level = level * jnp.repeat(heights, shape[position] // blocks).reshape([-1 if axis == position else 1 for axis in range(len(shape))])
    return level


def noise(own_key, shape, deviation, most, cuts=(), kind=jnp.bfloat16):
    drawn = deviation * jax.random.normal(own_key, shape, jnp.float32)
    if cuts:
        drawn = drawn * level_of(own_key, shape, cuts, -0.22, 0.18)
    return jnp.clip(drawn, -most, most).astype(kind)


def setup_inputs(seed: int = 0) -> dict:
    keys = jax.random.split(jax.random.key(seed), 14)
    tokens = noise(keys[0], (GROUPS, 2, SLOTS, D), 1.0, 6.0, ((0, 16), (1, 2)))
    text_segment = draw_text_segment(jax.random.fold_in(keys[13], 71), 0)
    ln1_gain = jnp.clip(1.0 + 0.1 * jax.random.normal(keys[2], (D,), jnp.float32), 0.5, 1.5)
    ln1_bias = noise(keys[3], (D,), 0.3, 3.0, (), jnp.float32)
    qkv_weight = noise(keys[4], (D, 3 * D), (D // 2) ** -0.5, 0.3125)
    out_weight = noise(keys[5], (D, D), (D // 8) ** -0.5, 0.625)
    attn_scale = jnp.clip(1.0 + 0.15 * jax.random.normal(keys[6], (D,), jnp.float32), 0.25, 1.75)
    ffn_scale = jnp.clip(1.0 + 0.15 * jax.random.normal(keys[7], (D,), jnp.float32), 0.25, 1.75)
    ln2_gain = jnp.clip(1.0 + 0.1 * jax.random.normal(keys[8], (2, D), jnp.float32), 0.5, 1.5)
    ln2_bias = noise(keys[9], (2, D), 0.3, 3.0, ((0, 2),), jnp.float32)
    expert_in = noise(keys[10], (2, D, FF), D ** -0.5, 0.21875, ((0, 2),))
    expert_out = noise(keys[11], (2, FF, D), (FF // 2) ** -0.5, 0.15625, ((0, 2),))
    out_cot = noise(keys[12], (GROUPS, 2, SLOTS, D), 1.0, 6.0, ((0, 16), (1, 2)))
    return {"tokens": tokens, "text_segment": text_segment, "ln1_gain": ln1_gain, "ln1_bias": ln1_bias, "qkv_weight": qkv_weight, "out_weight": out_weight, "attn_scale": attn_scale, "ffn_scale": ffn_scale, "ln2_gain": ln2_gain, "ln2_bias": ln2_bias, "expert_in": expert_in, "expert_out": expert_out, "out_cot": out_cot}


EPSILON = 1e-05
PRECISE = lax.Precision.HIGHEST

@jax.custom_vjp
def low(v):
    return lax.optimization_barrier(v.astype(jnp.bfloat16)).astype(jnp.float32)

@jax.custom_vjp
def low_back(v):
    return v

def low_keep(v):
    return (low(v), None)

def low_pass(kept, grad):
    return (grad,)

def back_keep(v):
    return (v, None)

def back_low(kept, grad):
    return (low(grad),)
low.defvjp(low_keep, low_pass)
low_back.defvjp(back_keep, back_low)

def layer_norm(inputs, gain_row, bias_row):
    row_mean = lax.optimization_barrier(jnp.mean(inputs, axis=-1, keepdims=True))
    centered = inputs - row_mean
    variance = lax.optimization_barrier(jnp.mean(centered * centered, axis=-1, keepdims=True))
    return centered * lax.rsqrt(variance + EPSILON) * gain_row + bias_row

def visibility(segments):
    batch, slot_count = segments.shape
    patch_key = jnp.arange(slot_count) < PATCHES
    text_key = segments < CAPTIONS
    same_caption = segments[:, :, None] == segments[:, None, :]
    patch_part = jnp.broadcast_to(patch_key[None, None, :], (batch, slot_count, slot_count))
    image_side = jnp.concatenate([patch_part, jnp.broadcast_to(text_key[:, None, :], (batch, slot_count, slot_count))], axis=2)
    text_side = jnp.concatenate([patch_part, same_caption], axis=2)
    return jnp.concatenate([image_side, text_side], axis=1)

def attend(block_items):
    queries, key_all, value_all, segments = block_items
    scores = jnp.einsum('bqhe,bkhe->bhqk', queries, key_all, precision=PRECISE) * HDIM ** (-0.5)
    scores = low_back(scores)
    visible = visibility(segments)[:, None, :, :]
    scores = jnp.where(visible, scores, jnp.float32(-1e+30))
    row_max = lax.optimization_barrier(jnp.max(scores, axis=-1, keepdims=True))
    exp_terms = jnp.exp(scores - row_max)
    weights = exp_terms / lax.optimization_barrier(jnp.sum(exp_terms, axis=-1, keepdims=True))
    mixed_heads = jnp.einsum('bhqk,bkhe->bqhe', low(weights), value_all, precision=PRECISE)
    return low_back(low(mixed_heads))

def forward(tokens, ln1_gain, ln1_bias, qkv_weight, out_weight, attn_scale, ffn_scale, ln2_gain, ln2_bias, expert_in, expert_out, text_segment):
    group_count = tokens.shape[0]
    flat_rows = tokens.reshape(group_count, 2 * SLOTS, D)
    attn_in = low(layer_norm(flat_rows, ln1_gain, ln1_bias))
    qkv = low_back(low(jnp.einsum('brd,de->bre', attn_in, qkv_weight, precision=PRECISE)))
    qkv = qkv.reshape(group_count // G_DEV, G_DEV, 2 * SLOTS, 3, HEADS, HDIM)
    segments = text_segment.reshape(group_count // G_DEV, G_DEV, SLOTS)
    mixed = lax.map(jax.checkpoint(attend), (qkv[:, :, :, 0], qkv[:, :, :, 1], qkv[:, :, :, 2], segments))
    mixed = mixed.reshape(group_count, 2 * SLOTS, D)
    attn_proj = low_back(jnp.einsum('brd,de->bre', mixed, out_weight, precision=PRECISE))
    residual = (flat_rows + attn_scale * attn_proj).reshape(group_count, 2, SLOTS, D)
    stream_outs = []
    for stream in range(2):
        stream_rows = residual[:, stream]
        ffn_in = low(layer_norm(stream_rows, ln2_gain[stream], ln2_bias[stream]))
        pre_act = low_back(jnp.einsum('bsd,df->bsf', ffn_in, expert_in[stream], precision=PRECISE))
        activation = low(jax.nn.gelu(pre_act, approximate=False))
        ffn_out = low_back(jnp.einsum('bsf,fd->bsd', activation, expert_out[stream], precision=PRECISE))
        stream_outs.append(stream_rows + ffn_scale * ffn_out)
    return jnp.stack(stream_outs, axis=1)

def reference(tokens, text_segment, ln1_gain, ln1_bias, qkv_weight, out_weight, attn_scale, ffn_scale, ln2_gain, ln2_bias, expert_in, expert_out, out_cot):
    float_args = (tokens.astype(jnp.float32), ln1_gain.astype(jnp.float32), ln1_bias.astype(jnp.float32), qkv_weight.astype(jnp.float32), out_weight.astype(jnp.float32), attn_scale.astype(jnp.float32), ffn_scale.astype(jnp.float32), ln2_gain.astype(jnp.float32), ln2_bias.astype(jnp.float32), expert_in.astype(jnp.float32), expert_out.astype(jnp.float32))

    def forward_fn(*inputs):
        return forward(*inputs, text_segment)
    result, pullback = jax.vjp(forward_fn, *float_args)
    gradients = pullback(out_cot.astype(jnp.float32))
    return (result.astype(jnp.bfloat16), gradients[0].astype(jnp.bfloat16), gradients[1], gradients[2], gradients[3], gradients[4], gradients[5], gradients[6], gradients[7], gradients[8], gradients[9], gradients[10])
```

```python
import functools

import jax
import jax.numpy as jnp
from jax import lax
from jax.experimental import pallas as pl
from jax.experimental.pallas import tpu as pltpu
from jax.sharding import PartitionSpec as P

HEADS = 12
HDIM = 64
PATCHES = 197
CAPTIONS = 5
EPSILON = 1e-05
LANES = 128
HIDDEN = -1e30
SCALE = HDIM ** (-0.5)
F32 = jnp.float32
BF16 = jnp.bfloat16


def layer_norm(inputs, gain_row, bias_row):
    row_mean = jnp.mean(inputs, axis=-1, keepdims=True)
    centered = inputs - row_mean
    variance = jnp.mean(centered * centered, axis=-1, keepdims=True)
    return centered * lax.rsqrt(variance + EPSILON) * gain_row + bias_row


def gelu_exact(inputs):
    return jax.nn.gelu(inputs, approximate=False)


def dot_nn(a, b):
    return lax.dot_general(a, b, (((1,), (0,)), ((), ())), preferred_element_type=F32)


def dot_nt(a, b):
    return lax.dot_general(a, b, (((1,), (1,)), ((), ())), preferred_element_type=F32)


def dot_tn(a, b):
    return lax.dot_general(a, b, (((0,), (0,)), ((), ())), preferred_element_type=F32)


def fill_bias(stream_ref, seg_row_ref, seg_col_ref, bias):
    slots = bias.shape[1]
    is_image = stream_ref[0] == 0
    seg_row = seg_row_ref[0]
    seg_col = seg_col_ref[0]
    key_slot = lax.broadcasted_iota(jnp.int32, (slots, slots), 0)
    patch = jnp.where(key_slot < PATCHES, 0.0, HIDDEN).astype(F32)
    text_col = jnp.where(seg_col < CAPTIONS, 0.0, HIDDEN).astype(F32)
    text = jnp.broadcast_to(text_col, (slots, slots))
    same = jnp.where(seg_col == seg_row, 0.0, HIDDEN).astype(F32)
    bias[0] = jnp.where(is_image, patch, same)
    bias[1] = jnp.where(is_image, text, patch)


def head_mask(shape, which):
    lane = lax.broadcasted_iota(jnp.int32, shape, 1)
    return (lane >= which * HDIM) & (lane < (which + 1) * HDIM)


def attend_kernel(stream_ref, seg_row_ref, seg_col_ref, qkv_ref, other_ref, mix_ref, lse_ref, bias):
    width = mix_ref.shape[2]
    fill_bias(stream_ref, seg_row_ref, seg_col_ref, bias)

    def pair_step(pair, carry):
        def cols(ref, part):
            return ref[0, :, pl.ds(pl.multiple_of(part * width + pair * LANES, LANES), LANES)]

        queries = cols(qkv_ref, 0) * jnp.asarray(SCALE, BF16)
        keys, values = cols(qkv_ref, 1), cols(qkv_ref, 2)
        keys_other, values_other = cols(other_ref, 0), cols(other_ref, 1)
        values_t, values_other_t = values.T, values_other.T
        mixed = []
        for which in range(2):
            q_head = jnp.where(head_mask(queries.shape, which), queries, jnp.zeros_like(queries))
            own = dot_nt(keys, q_head) + bias[0]
            other = dot_nt(keys_other, q_head) + bias[1]
            top = jnp.maximum(
                jnp.max(own, axis=0, keepdims=True), jnp.max(other, axis=0, keepdims=True)
            )
            own = jnp.exp(own - top)
            other = jnp.exp(other - top)
            total = jnp.sum(own, axis=0, keepdims=True) + jnp.sum(other, axis=0, keepdims=True)
            inverse = 1.0 / total
            lse_ref[0, pl.ds(pair * 2 + which, 1), :] = top + jnp.log(total)
            rows = slice(which * HDIM, (which + 1) * HDIM)
            mixed.append(
                dot_nn(values_t[rows], (own * inverse).astype(BF16))
                + dot_nn(values_other_t[rows], (other * inverse).astype(BF16))
            )
        mixed = jnp.concatenate(mixed, axis=0)
        mix_ref[0, :, pl.ds(pl.multiple_of(pair * LANES, LANES), LANES)] = mixed.T.astype(BF16)
        return carry

    lax.fori_loop(0, width // LANES, pair_step, 0)


def attend_back_kernel(
    stream_ref, seg_row_ref, seg_col_ref, qkv_ref, other_ref, gmix_ref, lse_ref, gq_ref, gkv_ref, bias
):
    width = gq_ref.shape[2]
    fill_bias(stream_ref, seg_row_ref, seg_col_ref, bias)

    def pair_step(pair, carry):
        def at(part):
            return pl.ds(pl.multiple_of(part * width + pair * LANES, LANES), LANES)

        queries = qkv_ref[0, :, at(0)] * jnp.asarray(SCALE, BF16)
        keys, values = qkv_ref[0, :, at(1)], qkv_ref[0, :, at(2)]
        keys_other, values_other = other_ref[0, :, at(0)], other_ref[0, :, at(1)]
        g_mix = gmix_ref[0, :, at(0)]
        keys_t, keys_other_t = keys.T, keys_other.T
        gq_t = []
        sums = [None] * 4
        for which in range(2):
            mask = head_mask(queries.shape, which)
            q_head = jnp.where(mask, queries, jnp.zeros_like(queries))
            g_head = jnp.where(mask, g_mix, jnp.zeros_like(g_mix))
            lse = lse_ref[0, pl.ds(pair * 2 + which, 1), :]
            p_own = jnp.exp(dot_nt(keys, q_head) + bias[0] - lse)
            p_other = jnp.exp(dot_nt(keys_other, q_head) + bias[1] - lse)
            gp_own = dot_nt(values, g_head)
            gp_other = dot_nt(values_other, g_head)
            inner = jnp.sum(p_own * gp_own, axis=0, keepdims=True) + jnp.sum(
                p_other * gp_other, axis=0, keepdims=True
            )
            ds_own = (p_own * (gp_own - inner)).astype(BF16)
            ds_other = (p_other * (gp_other - inner)).astype(BF16)
            rows = slice(which * HDIM, (which + 1) * HDIM)
            gq_t.append(dot_nn(keys_t[rows], ds_own) + dot_nn(keys_other_t[rows], ds_other))
            terms = [
                dot_nn(ds_own, q_head),
                dot_nn(p_own.astype(BF16), g_head),
                dot_nn(ds_other, q_head),
                dot_nn(p_other.astype(BF16), g_head),
            ]
            sums = [t if s is None else s + t for s, t in zip(sums, terms)]
        gq = jnp.concatenate(gq_t, axis=0).T * SCALE
        gq_ref[0, :, at(0)] = gq.astype(BF16)
        gkv_ref[0, 0, :, at(0)] = sums[0].astype(BF16)
        gkv_ref[0, 0, :, at(1)] = sums[1].astype(BF16)
        gkv_ref[1, 0, :, at(0)] = sums[2].astype(BF16)
        gkv_ref[1, 0, :, at(1)] = sums[3].astype(BF16)
        return carry

    lax.fori_loop(0, width // LANES, pair_step, 0)


def attention_specs(slots, width):
    return [
        pl.BlockSpec(memory_space=pltpu.SMEM),
        pl.BlockSpec((1, 1, slots), lambda g: (g, 0, 0)),
        pl.BlockSpec((1, slots, 1), lambda g: (g, 0, 0)),
        pl.BlockSpec((1, slots, 3 * width), lambda g: (g, 0, 0)),
        pl.BlockSpec((1, slots, 2 * width), lambda g: (g, 0, 0)),
    ]


def attend(stream, seg_row, seg_col, qkv, other):
    groups, slots, wide = qkv.shape
    width = wide // 3
    return pl.pallas_call(
        attend_kernel,
        grid=(groups,),
        in_specs=attention_specs(slots, width),
        out_specs=[
            pl.BlockSpec((1, slots, width), lambda g: (g, 0, 0)),
            pl.BlockSpec((1, 16, slots), lambda g: (g, 0, 0)),
        ],
        out_shape=[
            jax.ShapeDtypeStruct((groups, slots, width), BF16),
            jax.ShapeDtypeStruct((groups, 16, slots), F32),
        ],
        scratch_shapes=[pltpu.VMEM((2, slots, slots), F32)],
        compiler_params=pltpu.CompilerParams(vmem_limit_bytes=32 << 20),
        cost_estimate=pl.CostEstimate(
            flops=groups * 8 * slots * slots * width,
            bytes_accessed=groups * slots * width * 12,
            transcendentals=groups * HEADS * 2 * slots * slots,
        ),
        name="attend",
    )(stream, seg_row, seg_col, qkv, other)


def attend_back(stream, seg_row, seg_col, qkv, other, g_mix, lse):
    groups, slots, wide = qkv.shape
    width = wide // 3
    return pl.pallas_call(
        attend_back_kernel,
        grid=(groups,),
        in_specs=attention_specs(slots, width)
        + [
            pl.BlockSpec((1, slots, width), lambda g: (g, 0, 0)),
            pl.BlockSpec((1, 16, slots), lambda g: (g, 0, 0)),
        ],
        out_specs=[
            pl.BlockSpec((1, slots, width), lambda g: (g, 0, 0)),
            pl.BlockSpec((2, 1, slots, 2 * width), lambda g: (0, g, 0, 0)),
        ],
        out_shape=[
            jax.ShapeDtypeStruct((groups, slots, width), BF16),
            jax.ShapeDtypeStruct((2, groups, slots, 2 * width), BF16),
        ],
        scratch_shapes=[pltpu.VMEM((2, slots, slots), F32)],
        compiler_params=pltpu.CompilerParams(vmem_limit_bytes=32 << 20),
        cost_estimate=pl.CostEstimate(
            flops=groups * 20 * slots * slots * width,
            bytes_accessed=groups * slots * width * 24,
            transcendentals=groups * HEADS * 2 * slots * slots,
        ),
        name="attend_back",
    )(stream, seg_row, seg_col, qkv, other, g_mix, lse)


def shards(
    tokens,
    text_segment,
    ln1_gain,
    ln1_bias,
    qkv_weight,
    out_weight,
    attn_scale,
    ffn_scale,
    ln2_gain,
    ln2_bias,
    expert_in,
    expert_out,
    out_cot,
):
    groups, _, slots, width = tokens.shape
    rows = groups * slots
    swap = [(0, 1), (1, 0)]
    stream = lax.axis_index("stream").astype(jnp.int32).reshape(1)
    seg_row = text_segment.reshape(groups, 1, slots)
    seg_col = text_segment.reshape(groups, slots, 1)
    own_tokens = tokens.reshape(rows, width)
    other_tokens = lax.ppermute(own_tokens, "stream", swap)
    flat_rows = own_tokens.astype(F32)
    attn_in, ln1_pull = jax.vjp(layer_norm, flat_rows, ln1_gain, ln1_bias)
    attn_low = attn_in.astype(BF16)
    qkv = dot_nn(attn_low, qkv_weight).astype(BF16)
    other_low = layer_norm(other_tokens.astype(F32), ln1_gain, ln1_bias).astype(BF16)
    kv_weight = qkv_weight[:, width:]
    other_kv = dot_nn(other_low, kv_weight).astype(BF16)
    qkv = qkv.reshape(groups, slots, 3 * width)
    other_kv = other_kv.reshape(groups, slots, 2 * width)
    mixed, lse = attend(stream, seg_row, seg_col, qkv, other_kv)
    mixed = mixed.reshape(rows, width)
    attn_proj = dot_nn(mixed, out_weight)
    residual = flat_rows + attn_scale * attn_proj
    in_matrix = expert_in[0]
    out_matrix = expert_out[0]
    ffn_in, ln2_pull = jax.vjp(layer_norm, residual, ln2_gain[0], ln2_bias[0])
    ffn_low = ffn_in.astype(BF16)
    pre_act = dot_nn(ffn_low, in_matrix)
    activation = gelu_exact(pre_act).astype(BF16)
    ffn_out = dot_nn(activation, out_matrix)
    block_out = (residual + ffn_scale * ffn_out).astype(BF16)
    grad_out = out_cot.reshape(rows, width).astype(F32)
    ffn_scale_grad = jnp.sum(grad_out * ffn_out, axis=0)
    grad_ffn = (ffn_scale * grad_out).astype(BF16)
    expert_out_grad = dot_tn(activation, grad_ffn)
    grad_act = dot_nt(grad_ffn, out_matrix)
    _, gelu_pull = jax.vjp(gelu_exact, pre_act)
    grad_pre = gelu_pull(grad_act)[0].astype(BF16)
    expert_in_grad = dot_tn(ffn_low, grad_pre)
    grad_ffn_in = dot_nt(grad_pre, in_matrix)
    grad_resid_norm, ln2_gain_grad, ln2_bias_grad = ln2_pull(grad_ffn_in)
    grad_resid = grad_out + grad_resid_norm
    small_expert = jnp.stack([ln2_gain_grad, ln2_bias_grad], axis=0)
    expert_total = lax.psum(
        (expert_in_grad.astype(BF16), expert_out_grad.astype(BF16), small_expert.astype(BF16)), "dp"
    )
    attn_scale_grad = jnp.sum(grad_resid * attn_proj, axis=0)
    grad_proj = (attn_scale * grad_resid).astype(BF16)
    out_weight_grad = dot_tn(mixed, grad_proj)
    grad_mix = dot_nt(grad_proj, out_weight).astype(BF16).reshape(groups, slots, width)
    grad_query, grad_kv = attend_back(stream, seg_row, seg_col, qkv, other_kv, grad_mix, lse)
    grad_query = grad_query.reshape(rows, width)
    grad_kv = grad_kv.reshape(2, rows, 2 * width)
    back = dot_nt(grad_kv[1], kv_weight).astype(BF16)
    returned = lax.ppermute(back, "stream", swap)
    query_weight_grad = dot_tn(attn_low, grad_query)
    both_low = jnp.stack([attn_low, other_low], axis=0).reshape(2 * rows, width)
    kv_weight_grad = dot_tn(both_low, grad_kv.reshape(2 * rows, 2 * width))
    own_back = dot_nt(grad_query, qkv_weight[:, :width]) + dot_nt(grad_kv[0], kv_weight)
    grad_attn_in = own_back + returned.astype(F32)
    grad_rows_norm, ln1_gain_grad, ln1_bias_grad = ln1_pull(grad_attn_in)
    tokens_grad = (grad_resid + grad_rows_norm).astype(BF16).reshape(tokens.shape)
    small_grads = jnp.stack([ln1_gain_grad, ln1_bias_grad, attn_scale_grad, ffn_scale_grad], axis=0)
    shared_total = lax.psum(
        (
            query_weight_grad.astype(BF16),
            kv_weight_grad.astype(BF16),
            out_weight_grad.astype(BF16),
            small_grads.astype(BF16),
        ),
        ("dp", "stream"),
    )
    small_total = shared_total[3].astype(F32)
    small_expert = expert_total[2].astype(F32)
    qkv_weight_grad = jnp.concatenate([shared_total[0], shared_total[1]], axis=1).astype(F32)
    return (
        block_out.reshape(tokens.shape),
        tokens_grad,
        small_total[0],
        small_total[1],
        qkv_weight_grad,
        shared_total[2].astype(F32),
        small_total[2],
        small_total[3],
        small_expert[0][None, :],
        small_expert[1][None, :],
        expert_total[0].astype(F32)[None],
        expert_total[1].astype(F32)[None],
    )


def solution(mesh):
    rows4 = P("dp", "stream", None, None)
    ins = (
        rows4,
        P("dp", None),
        P(),
        P(),
        P(),
        P(),
        P(),
        P(),
        P("stream", None),
        P("stream", None),
        P("stream", None, None),
        P("stream", None, None),
        rows4,
    )
    outs = (
        rows4,
        rows4,
        P(),
        P(),
        P(),
        P(),
        P(),
        P(),
        P("stream", None),
        P("stream", None),
        P("stream", None, None),
        P("stream", None, None),
    )
    return jax.shard_map(shards, mesh=mesh, in_specs=ins, out_specs=outs, check_vma=False)
```

```python
import functools

import jax
import jax.numpy as jnp
from jax import lax
from jax.experimental import pallas as pl
from jax.experimental.pallas import tpu as pltpu
from jax.sharding import PartitionSpec as P

HEADS = 12
HDIM = 64
PATCHES = 197
CAPTIONS = 5
EPSILON = 1e-05
LANES = 128
HIDDEN = -1e30
SCALE = HDIM ** (-0.5)
F32 = jnp.float32
BF16 = jnp.bfloat16


def normalized(inputs):
    row_mean = jnp.mean(inputs, axis=-1, keepdims=True)
    centered = inputs - row_mean
    variance = jnp.mean(centered * centered, axis=-1, keepdims=True)
    inverse = lax.rsqrt(variance + EPSILON)
    return centered * inverse, inverse


def norm_input_grad(normed, inverse, gain_row, grad):
    scaled = grad * gain_row
    mean_scaled = jnp.mean(scaled, axis=-1, keepdims=True)
    mean_product = jnp.mean(scaled * normed, axis=-1, keepdims=True)
    return inverse * (scaled - mean_scaled - normed * mean_product)


def gelu_exact(inputs):
    return jax.nn.gelu(inputs, approximate=False)


def dot_nn(a, b):
    return lax.dot_general(a, b, (((1,), (0,)), ((), ())), preferred_element_type=F32)


def dot_nt(a, b):
    return lax.dot_general(a, b, (((1,), (1,)), ((), ())), preferred_element_type=F32)


def dot_tn(a, b):
    return lax.dot_general(a, b, (((0,), (0,)), ((), ())), preferred_element_type=F32)


def fill_bias(stream_ref, seg_row_ref, seg_col_ref, bias):
    slots = bias.shape[1]
    is_image = stream_ref[0] == 0
    seg_row = seg_row_ref[0]
    seg_col = seg_col_ref[0]
    key_slot = lax.broadcasted_iota(jnp.int32, (slots, slots), 0)
    patch = jnp.where(key_slot < PATCHES, 0.0, HIDDEN).astype(F32)
    text_col = jnp.where(seg_col < CAPTIONS, 0.0, HIDDEN).astype(F32)
    text = jnp.broadcast_to(text_col, (slots, slots))
    same = jnp.where(seg_col == seg_row, 0.0, HIDDEN).astype(F32)
    bias[0] = jnp.where(is_image, patch, same)
    bias[1] = jnp.where(is_image, text, patch)


def head_mask(shape, which):
    lane = lax.broadcasted_iota(jnp.int32, shape, 1)
    return (lane >= which * HDIM) & (lane < (which + 1) * HDIM)


def attend_kernel(stream_ref, seg_row_ref, seg_col_ref, qkv_ref, other_ref, mix_ref, lse_ref, bias):
    width = mix_ref.shape[2]
    fill_bias(stream_ref, seg_row_ref, seg_col_ref, bias)

    def pair_step(pair, carry):
        def cols(ref, part):
            return ref[0, :, pl.ds(pl.multiple_of(part * width + pair * LANES, LANES), LANES)]

        queries = cols(qkv_ref, 0) * jnp.asarray(SCALE, BF16)
        keys, values = cols(qkv_ref, 1), cols(qkv_ref, 2)
        keys_other, values_other = cols(other_ref, 0), cols(other_ref, 1)
        values_t, values_other_t = values.T, values_other.T
        mixed = []
        for which in range(2):
            q_head = jnp.where(head_mask(queries.shape, which), queries, jnp.zeros_like(queries))
            own = dot_nt(keys, q_head) + bias[0]
            other = dot_nt(keys_other, q_head) + bias[1]
            top = jnp.maximum(
                jnp.max(own, axis=0, keepdims=True), jnp.max(other, axis=0, keepdims=True)
            )
            own = jnp.exp(own - top)
            other = jnp.exp(other - top)
            total = jnp.sum(own, axis=0, keepdims=True) + jnp.sum(other, axis=0, keepdims=True)
            inverse = 1.0 / total
            lse_ref[0, pl.ds(pair * 2 + which, 1), :] = top + jnp.log(total)
            rows = slice(which * HDIM, (which + 1) * HDIM)
            mixed.append(
                dot_nn(values_t[rows], (own * inverse).astype(BF16))
                + dot_nn(values_other_t[rows], (other * inverse).astype(BF16))
            )
        mixed = jnp.concatenate(mixed, axis=0)
        mix_ref[0, :, pl.ds(pl.multiple_of(pair * LANES, LANES), LANES)] = mixed.T.astype(BF16)
        return carry

    lax.fori_loop(0, width // LANES, pair_step, 0)


def attend_back_kernel(
    stream_ref, seg_row_ref, seg_col_ref, qkv_ref, other_ref, gmix_ref, lse_ref, gq_ref, gkv_ref, bias
):
    width = gq_ref.shape[2]
    fill_bias(stream_ref, seg_row_ref, seg_col_ref, bias)

    def pair_step(pair, carry):
        def at(part):
            return pl.ds(pl.multiple_of(part * width + pair * LANES, LANES), LANES)

        queries = qkv_ref[0, :, at(0)] * jnp.asarray(SCALE, BF16)
        keys, values = qkv_ref[0, :, at(1)], qkv_ref[0, :, at(2)]
        keys_other, values_other = other_ref[0, :, at(0)], other_ref[0, :, at(1)]
        g_mix = gmix_ref[0, :, at(0)]
        keys_t, keys_other_t = keys.T, keys_other.T
        gq_t = []
        sums = [None] * 4
        for which in range(2):
            mask = head_mask(queries.shape, which)
            q_head = jnp.where(mask, queries, jnp.zeros_like(queries))
            g_head = jnp.where(mask, g_mix, jnp.zeros_like(g_mix))
            lse = lse_ref[0, pl.ds(pair * 2 + which, 1), :]
            p_own = jnp.exp(dot_nt(keys, q_head) + bias[0] - lse)
            p_other = jnp.exp(dot_nt(keys_other, q_head) + bias[1] - lse)
            gp_own = dot_nt(values, g_head)
            gp_other = dot_nt(values_other, g_head)
            inner = jnp.sum(p_own * gp_own, axis=0, keepdims=True) + jnp.sum(
                p_other * gp_other, axis=0, keepdims=True
            )
            ds_own = (p_own * (gp_own - inner)).astype(BF16)
            ds_other = (p_other * (gp_other - inner)).astype(BF16)
            rows = slice(which * HDIM, (which + 1) * HDIM)
            gq_t.append(dot_nn(keys_t[rows], ds_own) + dot_nn(keys_other_t[rows], ds_other))
            terms = [
                dot_nn(ds_own, q_head),
                dot_nn(p_own.astype(BF16), g_head),
                dot_nn(ds_other, q_head),
                dot_nn(p_other.astype(BF16), g_head),
            ]
            sums = [t if s is None else s + t for s, t in zip(sums, terms)]
        gq = jnp.concatenate(gq_t, axis=0).T * SCALE
        gq_ref[0, :, at(0)] = gq.astype(BF16)
        gkv_ref[0, 0, :, at(0)] = sums[0].astype(BF16)
        gkv_ref[0, 0, :, at(1)] = sums[1].astype(BF16)
        gkv_ref[1, 0, :, at(0)] = sums[2].astype(BF16)
        gkv_ref[1, 0, :, at(1)] = sums[3].astype(BF16)
        return carry

    lax.fori_loop(0, width // LANES, pair_step, 0)


def attention_specs(slots, width):
    return [
        pl.BlockSpec(memory_space=pltpu.SMEM),
        pl.BlockSpec((1, 1, slots), lambda g: (g, 0, 0)),
        pl.BlockSpec((1, slots, 1), lambda g: (g, 0, 0)),
        pl.BlockSpec((1, slots, 3 * width), lambda g: (g, 0, 0)),
        pl.BlockSpec((1, slots, 2 * width), lambda g: (g, 0, 0)),
    ]


def attend(stream, seg_row, seg_col, qkv, other):
    groups, slots, wide = qkv.shape
    width = wide // 3
    return pl.pallas_call(
        attend_kernel,
        grid=(groups,),
        in_specs=attention_specs(slots, width),
        out_specs=[
            pl.BlockSpec((1, slots, width), lambda g: (g, 0, 0)),
            pl.BlockSpec((1, 16, slots), lambda g: (g, 0, 0)),
        ],
        out_shape=[
            jax.ShapeDtypeStruct((groups, slots, width), BF16),
            jax.ShapeDtypeStruct((groups, 16, slots), F32),
        ],
        scratch_shapes=[pltpu.VMEM((2, slots, slots), F32)],
        compiler_params=pltpu.CompilerParams(vmem_limit_bytes=32 << 20),
        cost_estimate=pl.CostEstimate(
            flops=groups * 8 * slots * slots * width,
            bytes_accessed=groups * slots * width * 12,
            transcendentals=groups * HEADS * 2 * slots * slots,
        ),
        name="attend",
    )(stream, seg_row, seg_col, qkv, other)


def attend_back(stream, seg_row, seg_col, qkv, other, g_mix, lse):
    groups, slots, wide = qkv.shape
    width = wide // 3
    return pl.pallas_call(
        attend_back_kernel,
        grid=(groups,),
        in_specs=attention_specs(slots, width)
        + [
            pl.BlockSpec((1, slots, width), lambda g: (g, 0, 0)),
            pl.BlockSpec((1, 16, slots), lambda g: (g, 0, 0)),
        ],
        out_specs=[
            pl.BlockSpec((1, slots, width), lambda g: (g, 0, 0)),
            pl.BlockSpec((2, 1, slots, 2 * width), lambda g: (0, g, 0, 0)),
        ],
        out_shape=[
            jax.ShapeDtypeStruct((groups, slots, width), BF16),
            jax.ShapeDtypeStruct((2, groups, slots, 2 * width), BF16),
        ],
        scratch_shapes=[pltpu.VMEM((2, slots, slots), F32)],
        compiler_params=pltpu.CompilerParams(vmem_limit_bytes=32 << 20),
        cost_estimate=pl.CostEstimate(
            flops=groups * 20 * slots * slots * width,
            bytes_accessed=groups * slots * width * 24,
            transcendentals=groups * HEADS * 2 * slots * slots,
        ),
        name="attend_back",
    )(stream, seg_row, seg_col, qkv, other, g_mix, lse)


class Plan:
    def __init__(self, dp, streams):
        self.outer = 4
        self.inner = max(dp // 8, 1)
        self.dp = dp
        self.streams = streams

    def pieces(self, partials):
        if self.dp != 2 * self.outer * self.inner:
            return None
        pieces = []
        for array, shared, cuts in zip(partials, SHARED, CUTS):
            piece = array.shape[0] // cuts
            parts = self.inner * self.outer * (self.streams if shared else 1)
            if array.shape[0] % cuts or piece % (16 * parts) or array.shape[1] % (2 * LANES):
                return None
            pieces.append(piece)
        return pieces


def add_rows(target, first, others, rows):
    step = 16
    for candidate in (64, 48, 32):
        if rows % candidate == 0:
            step = candidate
            break

    def band(i, carry):
        at = pl.ds(pl.multiple_of(i * step, step), step)
        total = first[at, :].astype(F32)
        for ref in others:
            total = total + ref[at, :].astype(F32)
        target[at, :] = total.astype(target.dtype)
        return carry

    lax.fori_loop(0, rows // step, band, 0)


def job_levels(plan, shared):
    levels = [("inner", plan.inner), ("outer", plan.outer)]
    return ([("stream", plan.streams)] if shared else []) + levels


def job_scratch(plan, job):
    rows, half, shared = job[2], job[3] // 2, job[4]
    shapes = [pltpu.VMEM((rows, half), BF16), pltpu.VMEM((rows, half), BF16)]
    for _, size in job_levels(plan, shared):
        rows = rows // size
        shapes.append(pltpu.VMEM((size - 1, rows, half), BF16))
        shapes.append(pltpu.VMEM((rows, half), BF16))
    copies = 2 + 2 * sum(size - 1 for _, size in job_levels(plan, shared))
    shapes += [
        pltpu.SemaphoreType.DMA((copies,)),
        pltpu.SemaphoreType.DMA((copies,)),
        pltpu.SemaphoreType.DMA((2,)),
    ]
    return shapes


def reduce_kernel(plan, jobs, count, *refs):
    ins, small_in = refs[:count], refs[count]
    outs, small_out = refs[count + 1 : 2 * count + 1], refs[2 * count + 1]
    scratch = list(refs[2 * count + 2 :])
    dp_index, stream_index = lax.axis_index("dp"), lax.axis_index("stream")
    place = {
        "core": dp_index % 2,
        "inner": (dp_index // 2) % plan.inner,
        "outer": dp_index // (2 * plan.inner),
        "stream": stream_index,
    }
    sizes = {"core": 2, "inner": plan.inner, "outer": plan.outer, "stream": plan.streams}

    def peer(axis, offset):
        at = dict(place)
        at[axis] = (place[axis] + offset) % sizes[axis]
        dp = (at["outer"] * plan.inner + at["inner"]) * 2 + at["core"]
        return (dp, at["stream"]), at[axis]

    barrier = pltpu.get_barrier_semaphore()
    neighbours = [peer(axis, o)[0] for axis in sizes for o in range(1, sizes[axis])]
    for device in neighbours:
        pl.semaphore_signal(barrier, inc=1, device_id=device, device_id_type=pl.DeviceIdType.MESH)
    pl.semaphore_wait(barrier, len(neighbours))
    sent = []

    def send(source, target, send_sem, recv_sem, device):
        copy = pltpu.make_async_remote_copy(
            src_ref=source,
            dst_ref=target,
            send_sem=send_sem,
            recv_sem=recv_sem,
            device_id=device,
            device_id_type=pl.DeviceIdType.MESH,
        )
        copy.start()
        sent.append(copy)
        return copy

    def job_stages(job):
        array, start, rows, columns, shared = job
        half = columns // 2
        levels = job_levels(plan, shared)
        mine, partner = scratch.pop(0), scratch.pop(0)
        stages_refs = [(scratch.pop(0), scratch.pop(0)) for _ in levels]
        send_sems, recv_sems, local_sems = scratch.pop(0), scratch.pop(0), scratch.pop(0)
        source, result = ins[array], outs[array]
        own_columns = pl.ds(pl.multiple_of(place["core"] * half, half), half)
        far_columns = pl.ds(pl.multiple_of((1 - place["core"]) * half, half), half)
        state = {"slot": 0}
        waits = {}

        def next_slot():
            state["slot"] += 1
            return state["slot"] - 1

        def begin():
            slot = next_slot()
            device, _ = peer("core", 1)
            waits["core"] = send(
                source.at[pl.ds(start, rows), far_columns], partner, send_sems.at[slot], recv_sems.at[slot], device
            )
            waits["local"] = pltpu.make_async_copy(
                source.at[pl.ds(start, rows), own_columns], mine, local_sems.at[0]
            )
            waits["local"].start()

        def spread(index, held, held_rows):
            axis, size = levels[index]
            part = held_rows // size
            waits[index] = []
            for offset in range(1, size):
                slot = next_slot()
                device, target = peer(axis, offset)
                rows_at = pl.ds(pl.multiple_of(target * part, part), part)
                waits[index].append(
                    send(
                        held.at[rows_at, :],
                        stages_refs[index][0].at[offset - 1],
                        send_sems.at[slot],
                        recv_sems.at[slot],
                        device,
                    )
                )

        def first_sum():
            waits["local"].wait()
            waits["core"].wait_recv()
            add_rows(mine, mine, [partner], rows)
            spread(0, mine, rows)

        def held_before(index):
            return (mine, rows) if index == 0 else (stages_refs[index - 1][1], rows_before[index])

        rows_before = [rows]
        for _, size in levels:
            rows_before.append(rows_before[-1] // size)

        def level_sum(index):
            axis, size = levels[index]
            held = held_before(index)[0]
            part = rows_before[index + 1]
            received, total = stages_refs[index]
            for copy in waits[index]:
                copy.wait_recv()
            own = held.at[pl.ds(pl.multiple_of(place[axis] * part, part), part), :]
            add_rows(total, own, [received.at[o] for o in range(size - 1)], part)

        def gathered(index):
            offset = start
            for level in range(index):
                offset = offset + place[levels[level][0]] * rows_before[level + 1]
            return pl.ds(pl.multiple_of(offset, 16), rows_before[index])

        def gather(index, held):
            axis, size = levels[index]
            region = result.at[gathered(index + 1), own_columns]
            waits[("gather", index)] = []
            for offset in range(1, size):
                slot = next_slot()
                device, _ = peer(axis, offset)
                waits[("gather", index)].append(
                    send(held if held is not None else region, region, send_sems.at[slot], recv_sems.at[slot], device)
                )

        def wait_gather(index):
            for copy in waits[("gather", index)]:
                copy.wait_recv()

        last = len(levels) - 1
        stages = [begin, first_sum]
        for index in range(last):
            def middle(index=index):
                level_sum(index)
                spread(index + 1, stages_refs[index][1], rows_before[index + 1])
            stages.append(middle)

        def turn():
            level_sum(last)
            total = stages_refs[last][1]
            gather(last, total)
            waits["out"] = pltpu.make_async_copy(
                total, result.at[gathered(last + 1), own_columns], local_sems.at[1]
            )
            waits["out"].start()

        stages.append(turn)
        for index in range(last, 0, -1):
            def up(index=index):
                wait_gather(index)
                if index == last:
                    waits["out"].wait()
                gather(index - 1, None)
            stages.append(up)

        def core_gather():
            wait_gather(0)
            slot = next_slot()
            device, _ = peer("core", 1)
            region = result.at[pl.ds(start, rows), own_columns]
            waits["back"] = send(region, region, send_sems.at[slot], recv_sems.at[slot], device)

        def finish():
            waits["back"].wait_recv()

        return stages + [core_gather, finish]

    def small_stages():
        rows, columns = small_in.shape
        order = ["core", "stream", "inner", "outer"]
        held = [scratch.pop(0) for _ in order]
        own, local = scratch.pop(0), scratch.pop(0)
        send_sems, recv_sems = scratch.pop(0), scratch.pop(0)
        slot = 0
        stages = []
        plans = []
        for axis in order:
            plans.append((axis, [slot + i for i in range(sizes[axis] - 1)]))
            slot += sizes[axis] - 1
        pending = {}

        def share(index, value_ref):
            axis, slots = plans[index]
            pending[index] = []
            for offset, at in enumerate(slots, 1):
                device, _ = peer(axis, offset)
                pending[index].append(
                    send(value_ref, held[index].at[offset - 1], send_sems.at[at], recv_sems.at[at], device)
                )

        def collect(index, value_ref):
            axis, _ = plans[index]
            size = sizes[axis]
            for copy in pending[index]:
                copy.wait_recv()
            total = None
            for member in range(size):
                term = jnp.where(place[axis] == member, value_ref[...], jnp.zeros(value_ref.shape, F32))
                for offset in range(1, size):
                    is_there = (member + offset) % size == place[axis]
                    term = term + jnp.where(is_there, held[index][offset - 1], jnp.zeros(value_ref.shape, F32))
                total = term if total is None else total + term
            return total

        def begin():
            share(0, small_in)

        def step(index):
            value_ref = small_in if index == 0 else own.at[index - 1]
            own[index] = collect(index, value_ref)
            share(index + 1, own.at[index])

        def finish():
            small_out[...] = collect(len(order) - 1, own.at[len(order) - 2])

        stages = [begin]
        for index in range(len(order) - 1):
            stages.append(functools.partial(step, index))
        return stages + [finish]

    pipelines = [job_stages(job) for job in jobs]
    small = small_stages()
    small[0]()
    for stages in pipelines:
        stages[0]()
    starts = [0] * len(pipelines)
    tick = {False: 0, True: 0}
    for i, job in enumerate(jobs):
        starts[i] = tick[job[4]]
        tick[job[4]] += 1
    last_tick = max(s + len(p) for s, p in zip(starts, pipelines))
    for now in range(last_tick):
        for begin_at, stages in zip(starts, pipelines):
            at = now - begin_at + 1
            if 1 <= at < len(stages):
                stages[at]()
        if 1 <= now + 1 < len(small):
            small[now + 1]()
    for copy in sent:
        copy.wait_send()


def reduce_jobs(arrays, shared_flags, pieces):
    expert, common = [], []
    for index, (array, shared, piece) in enumerate(zip(arrays, shared_flags, pieces)):
        rows, columns = array.shape
        for start in range(0, rows, piece):
            (common if shared else expert).append((index, start, piece, columns, shared))
    merged = []
    while expert or common:
        if expert:
            merged.append(expert.pop(0))
        if common:
            merged.append(common.pop(0))
    return merged


def reduce_all(plan, arrays, shared_flags, pieces, small):
    jobs = reduce_jobs(arrays, shared_flags, pieces)
    scratch = []
    for job in jobs:
        scratch += job_scratch(plan, job)
    small_shape = small.shape
    sizes = [2, plan.streams, plan.inner, plan.outer]
    scratch += [pltpu.VMEM((max(size - 1, 1),) + small_shape, F32) for size in sizes]
    scratch += [pltpu.VMEM((4,) + small_shape, F32), pltpu.VMEM(small_shape, F32)]
    copies = sum(size - 1 for size in sizes)
    scratch += [pltpu.SemaphoreType.DMA((copies,)), pltpu.SemaphoreType.DMA((copies,))]
    anywhere = pl.BlockSpec(memory_space=pl.ANY)
    in_vmem = pl.BlockSpec(memory_space=pltpu.VMEM)
    result = pl.pallas_call(
        functools.partial(reduce_kernel, plan, jobs, len(arrays)),
        in_specs=[anywhere] * len(arrays) + [in_vmem],
        out_specs=[anywhere] * len(arrays) + [in_vmem],
        out_shape=[jax.ShapeDtypeStruct(a.shape, a.dtype) for a in arrays]
        + [jax.ShapeDtypeStruct(small_shape, F32)],
        scratch_shapes=scratch,
        compiler_params=pltpu.CompilerParams(
            collective_id=0, has_side_effects=True, vmem_limit_bytes=56 << 20
        ),
        name="reduce_all",
    )(*arrays, small)
    return result[:-1], result[-1]

SHARED = (False, False, True, True, True)
CUTS = (3, 3, 3, 1, 1)


def reduce_partials(plan, partials, small):
    pieces = plan.pieces(partials)
    if pieces is not None:
        return reduce_all(plan, partials, SHARED, pieces, small)
    everyone = ("dp", "stream")
    totals = [lax.psum(p, everyone if shared else "dp") for p, shared in zip(partials, SHARED)]
    return totals, lax.psum(small, everyone)


def shards(
    plan,
    tokens,
    text_segment,
    ln1_gain,
    ln1_bias,
    qkv_weight,
    out_weight,
    attn_scale,
    ffn_scale,
    ln2_gain,
    ln2_bias,
    expert_in,
    expert_out,
    out_cot,
):
    groups, _, slots, width = tokens.shape
    rows = groups * slots
    swap = [(0, 1), (1, 0)]
    stream = lax.axis_index("stream").astype(jnp.int32).reshape(1)
    seg_row = text_segment.reshape(groups, 1, slots)
    seg_col = text_segment.reshape(groups, slots, 1)
    own_tokens = tokens.reshape(rows, width)
    other_tokens = lax.ppermute(own_tokens, "stream", swap)
    flat_rows = own_tokens.astype(F32)
    normed, inverse = normalized(flat_rows)
    attn_low = (normed * ln1_gain + ln1_bias).astype(BF16)
    qkv = dot_nn(attn_low, qkv_weight).astype(BF16)
    other_normed, _ = normalized(other_tokens.astype(F32))
    other_low = (other_normed * ln1_gain + ln1_bias).astype(BF16)
    kv_weight = qkv_weight[:, width:]
    other_kv = dot_nn(other_low, kv_weight).astype(BF16)
    qkv = qkv.reshape(groups, slots, 3 * width)
    other_kv = other_kv.reshape(groups, slots, 2 * width)
    mixed, lse = attend(stream, seg_row, seg_col, qkv, other_kv)
    mixed = mixed.reshape(rows, width)
    attn_proj = dot_nn(mixed, out_weight)
    residual = flat_rows + attn_scale * attn_proj
    in_matrix = expert_in[0]
    out_matrix = expert_out[0]
    normed2, inverse2 = normalized(residual)
    ffn_low = (normed2 * ln2_gain[0] + ln2_bias[0]).astype(BF16)
    pre_act = dot_nn(ffn_low, in_matrix)
    activation = gelu_exact(pre_act).astype(BF16)
    ffn_out = dot_nn(activation, out_matrix)
    block_out = (residual + ffn_scale * ffn_out).astype(BF16)
    grad_out = out_cot.reshape(rows, width).astype(F32)
    ffn_scale_grad = jnp.sum(grad_out * ffn_out, axis=0)
    grad_ffn = (ffn_scale * grad_out).astype(BF16)
    expert_out_grad = dot_tn(activation, grad_ffn)
    grad_act = dot_nt(grad_ffn, out_matrix)
    _, gelu_pull = jax.vjp(gelu_exact, pre_act)
    grad_pre = gelu_pull(grad_act)[0].astype(BF16)
    expert_in_grad = dot_tn(ffn_low, grad_pre)
    grad_ffn_in = dot_nt(grad_pre, in_matrix)
    ln2_gain_grad = jnp.sum(grad_ffn_in * normed2, axis=0)
    ln2_bias_grad = jnp.sum(grad_ffn_in, axis=0)
    grad_resid = grad_out + norm_input_grad(normed2, inverse2, ln2_gain[0], grad_ffn_in)
    attn_scale_grad = jnp.sum(grad_resid * attn_proj, axis=0)
    grad_proj = (attn_scale * grad_resid).astype(BF16)
    out_weight_grad = dot_tn(mixed, grad_proj)
    grad_mix = dot_nt(grad_proj, out_weight).astype(BF16).reshape(groups, slots, width)
    grad_query, grad_kv = attend_back(stream, seg_row, seg_col, qkv, other_kv, grad_mix, lse)
    grad_query = grad_query.reshape(rows, width)
    grad_kv = grad_kv.reshape(2, rows, 2 * width)
    other_back = dot_nt(grad_kv[1], kv_weight)
    returned = lax.ppermute(other_back.astype(BF16), "stream", swap)
    query_weight_grad = dot_tn(attn_low, grad_query)
    both_low = jnp.stack([attn_low, other_low], axis=0).reshape(2 * rows, width)
    kv_weight_grad = dot_tn(both_low, grad_kv.reshape(2 * rows, 2 * width))
    own_back = dot_nt(grad_query, qkv_weight[:, :width]) + dot_nt(grad_kv[0], kv_weight)
    ln1_gain_grad = jnp.sum(own_back * normed, axis=0) + jnp.sum(other_back * other_normed, axis=0)
    ln1_bias_grad = jnp.sum(own_back, axis=0) + jnp.sum(other_back, axis=0)
    here = lax.broadcasted_iota(jnp.int32, (plan.streams, 1), 0) == stream
    small = jnp.concatenate(
        [
            jnp.stack([ln1_gain_grad, ln1_bias_grad, attn_scale_grad, ffn_scale_grad], axis=0),
            jnp.where(here, ln2_gain_grad[None], 0.0),
            jnp.where(here, ln2_bias_grad[None], 0.0),
        ],
        axis=0,
    )
    partials = [
        expert_in_grad.astype(BF16),
        expert_out_grad.astype(BF16),
        kv_weight_grad.astype(BF16),
        query_weight_grad.astype(BF16),
        out_weight_grad.astype(BF16),
    ]
    totals, small_total = reduce_partials(plan, partials, small)
    grad_attn_in = own_back + returned.astype(F32)
    grad_rows_norm = norm_input_grad(normed, inverse, ln1_gain, grad_attn_in)
    tokens_grad = (grad_resid + grad_rows_norm).astype(BF16).reshape(tokens.shape)
    expert_in_total, expert_out_total, kv_total, query_total, out_total = totals
    ln2_gain_total = jnp.sum(jnp.where(here, small_total[4 : 4 + plan.streams], 0.0), axis=0)
    ln2_bias_total = jnp.sum(jnp.where(here, small_total[4 + plan.streams :], 0.0), axis=0)
    return (
        block_out.reshape(tokens.shape),
        tokens_grad,
        small_total[0],
        small_total[1],
        jnp.concatenate([query_total, kv_total], axis=1).astype(F32),
        out_total.astype(F32),
        small_total[2],
        small_total[3],
        ln2_gain_total[None],
        ln2_bias_total[None],
        expert_in_total.astype(F32)[None],
        expert_out_total.astype(F32)[None],
    )


def solution(mesh):
    rows4 = P("dp", "stream", None, None)
    ins = (
        rows4,
        P("dp", None),
        P(),
        P(),
        P(),
        P(),
        P(),
        P(),
        P("stream", None),
        P("stream", None),
        P("stream", None, None),
        P("stream", None, None),
        rows4,
    )
    outs = (
        rows4,
        rows4,
        P(),
        P(),
        P(),
        P(),
        P(),
        P(),
        P("stream", None),
        P("stream", None),
        P("stream", None, None),
        P("stream", None, None),
    )
    plan = Plan(mesh.shape["dp"], mesh.shape["stream"])
    return jax.shard_map(functools.partial(shards, plan), mesh=mesh, in_specs=ins, out_specs=outs, check_vma=False)
```
